32 devices in a mesh: row: 8 (over y, x, core), col: 4 (over z).
Axes of the slice: x: 2, y: 2, z: 4, core: 2. Of those that a mesh axis runs over, the one named last changes fastest.
Arguments:
- tokens: bfloat16 [1024, 8192], P('row', 'col'), may hold values from -200 to 200
- norm_gain: float32 [8192], P('col'), may hold values from 0.1 to 1.9
- gate_weight: bfloat16 [8192, 28672], P('col', 'row'), may hold values from -0.0625 to 0.0625
- up_weight: bfloat16 [8192, 28672], P('col', 'row'), may hold values from -0.0625 to 0.0625
- down_weight: bfloat16 [28672, 8192], P('row', 'col'), may hold values from -0.03125 to 0.03125
Outputs:
- mixed: bfloat16 [1024, 8192], P('row', 'col')
The draws below stay inside these ranges and needn't reach their ends.
All inputs are finite; a program needn't handle non-finite values.
Results may differ from the reference program's by a relative error of at most 0.028.
Values may be sent and summed in bfloat16 or wider, within the bound.
No kernel may reach another device: no remote copies, remote signals or barrier semaphores. Data moves between devices by JAX's collectives and lax.ppermute only.
A program may use at most 128 MiB of HBM per device.

```python
import math
import jax
import jax.numpy as jnp
from jax import lax

D = 8192
FF = 28672
TOKENS = 1024
N_ROW = 8
N_COL = 4


def draw_tokens(key, part):
    first, second, third = jax.random.split(jax.random.fold_in(key, 11), 3)
    ramp = jnp.sqrt(1.0 + 2.0 * jnp.arange(D, dtype=jnp.float32) / max(D - 1, 1))
    rough = jnp.exp(jax.random.uniform(second, (D,), jnp.float32, -0.35, 0.35))
    column_scale = ramp * rough
    base = jax.random.normal(first, (TOKENS, D), jnp.float32)
    row_scale = jnp.exp(jax.random.uniform(third, (TOKENS, 1), jnp.float32, 0.0, math.log(10.0)))
    values = jnp.clip(base * column_scale[None, :] * row_scale, -200.0, 200.0)
    return values.astype(jnp.bfloat16)


def level_of(rng, extent, shards, least, largest):
    factor_of = 1.0
    for axis_at, blocks in shards:
        heights = jax.random.uniform(jax.random.fold_in(jax.random.fold_in(rng, 6), axis_at), (blocks,), jnp.float32, least / len(shards), largest / len(shards))
        factor_of = factor_of * jnp.repeat(jnp.exp(heights), extent[axis_at] // blocks).reshape((-1,) + (1,) * (len(extent) - 1 - axis_at))
    return factor_of


def gaussian(stream_key, extent, width, most, cuts=(), kind=jnp.bfloat16):
    level = level_of(stream_key, extent, cuts, -0.22, 0.18) if cuts else 1.0
    array = jax.random.normal(stream_key, extent, jnp.float32) * width * level
    return jnp.minimum(jnp.maximum(array, -most), most).astype(kind)


def setup_inputs(seed: int = 0) -> dict:
    streams_of = jax.random.split(jax.random.key(seed), 6)
    tokens = draw_tokens(jax.random.fold_in(streams_of[5], 71), 0)
    norm_gain = jnp.clip(1.0 + 0.18 * jax.random.normal(streams_of[1], (D,), jnp.float32), 0.1, 1.9)
    gate_weight = gaussian(streams_of[2], (D, FF), D ** -0.5, 0.0625, ((0, 4), (1, 8)))
    up_weight = gaussian(streams_of[3], (D, FF), D ** -0.5, 0.0625, ((0, 4), (1, 8)))
    down_weight = gaussian(streams_of[4], (FF, D), FF ** -0.5, 0.03125, ((0, 8), (1, 4)))
    return {"tokens": tokens, "norm_gain": norm_gain, "gate_weight": gate_weight, "up_weight": up_weight, "down_weight": down_weight}


def reference(tokens, norm_gain, gate_weight, up_weight, down_weight):
    values = tokens.astype(jnp.float32)
    squares = lax.optimization_barrier(jnp.sum(values * values, axis=1))
    scale = lax.rsqrt(squares / D + 1e-05)
    normed = (values * scale[:, None] * norm_gain[None, :]).astype(jnp.bfloat16)
    group = D // N_COL
    gate = jnp.zeros((TOKENS, FF), jnp.float32)
    up = jnp.zeros((TOKENS, FF), jnp.float32)
    for index in range(N_COL):
        rows = normed[:, index * group:(index + 1) * group]
        part_gate = jnp.dot(rows, gate_weight[index * group:(index + 1) * group], preferred_element_type=jnp.float32)
        part_up = jnp.dot(rows, up_weight[index * group:(index + 1) * group], preferred_element_type=jnp.float32)
        gate = gate + part_gate.astype(jnp.bfloat16).astype(jnp.float32)
        up = up + part_up.astype(jnp.bfloat16).astype(jnp.float32)
    hidden = (jax.nn.silu(gate) * up).astype(jnp.bfloat16)
    hgroup = FF // N_ROW
    mixed = jnp.zeros((TOKENS, D), jnp.float32)
    for index in range(N_ROW):
        part = jnp.dot(hidden[:, index * hgroup:(index + 1) * hgroup], down_weight[index * hgroup:(index + 1) * hgroup], preferred_element_type=jnp.float32)
        mixed = mixed + part.astype(jnp.bfloat16).astype(jnp.float32)
    return mixed.astype(jnp.bfloat16)
```

```python
import functools

import jax
import jax.numpy as jnp
from jax import lax
from jax.experimental import pallas as pl
from jax.experimental.pallas import tpu as pltpu
from jax.sharding import PartitionSpec as P


FIRST = (2, 2)
SECOND = (4, 3)
MIDDLE = (4, 3)
LAST = (2, 1)
AHEAD = 3
ROW_TILE = 32
KERNEL_VMEM = 52 * 2**20
SMALL_VMEM = 8 * 2**20


HBM = pl.BlockSpec(memory_space=pltpu.HBM)
VMEM = pl.BlockSpec(memory_space=pltpu.VMEM)
SMEM = pl.BlockSpec(memory_space=pltpu.SMEM)
ANY = pl.BlockSpec(memory_space=pl.ANY)


def gate_up_kernel(blocks, start, unit, off_ref, x_ref, gate_hbm, up_hbm, far_ref, near_ref):
    def step(gate_ref, up_ref):
        i = pl.program_id(0)
        x = x_ref[...]
        gate = jnp.dot(x, gate_ref[...], preferred_element_type=jnp.float32).astype(jnp.bfloat16)
        up = jnp.dot(x, up_ref[...], preferred_element_type=jnp.float32).astype(jnp.bfloat16)

        def write(ref, u):
            at = pl.multiple_of(2 * unit * u, 2 * unit)
            ref[:, pl.ds(at, unit)] = gate
            ref[:, pl.ds(at + unit, unit)] = up

        pl.when(i < blocks)(lambda: write(far_ref, i))
        pl.when(i >= blocks)(lambda: write(near_ref, i - blocks))

    def weight_at(i):
        return 0, off_ref[i // blocks] + start + i - (i // blocks) * blocks

    weight = pl.BlockSpec((x_ref.shape[1], unit), weight_at)
    pltpu.emit_pipeline(step, grid=(2 * blocks,), in_specs=[weight, weight])(gate_hbm, up_hbm)


def gate_up(x, gate_weight, up_weight, offsets, start, blocks, unit):
    rows, depth = x.shape
    shape = jax.ShapeDtypeStruct((rows, 2 * blocks * unit), jnp.bfloat16)
    return pl.pallas_call(
        functools.partial(gate_up_kernel, blocks, start, unit),
        in_specs=[SMEM, VMEM, HBM, HBM],
        out_specs=[VMEM, VMEM],
        out_shape=[shape, shape],
        compiler_params=pltpu.CompilerParams(vmem_limit_bytes=KERNEL_VMEM),
        cost_estimate=pl.CostEstimate(
            flops=8 * rows * depth * blocks * unit,
            bytes_accessed=8 * depth * blocks * unit,
            transcendentals=0,
        ),
    )(offsets, x, gate_weight, up_weight)


def down_kernel(steps, starts, places, unit, n_roles, has_total, off_ref, weight_hbm, *refs):
    out_ref, acc_ref = refs[-2:]
    rows, width = out_ref.shape
    count = sum(size for _, _, _, size in steps)
    acc_ref[...] = refs[-3][...] if has_total else jnp.zeros_like(acc_ref)

    def weight_at(k):
        index = 0
        for flow, chunk, first, size in steps:
            index = jnp.where(k >= first, off_ref[1 - flow] + starts[chunk] + k - first, index)
        return index, 0

    def run(role):
        def step(weight_ref, *pieces):
            k = pl.program_id(0)
            for (flow, chunk, first, size), ref in zip(steps, pieces):
                @pl.when((k >= first) & (k < first + size))
                def _():
                    acc_ref[...] += jnp.dot(ref[...], weight_ref[...], preferred_element_type=jnp.float32)

        specs, operands = [pl.BlockSpec((unit, width), weight_at)], [weight_hbm]
        for flow, chunk, first, size in steps:
            index = (2 * chunk + flow) * n_roles + role
            at = places[index]
            specs.append(pl.BlockSpec(
                (rows, unit),
                lambda k, at=at, first=first, size=size: (0, at + jnp.clip(k - first, 0, size - 1)),
            ))
            operands.append(refs[index])
        pltpu.emit_pipeline(step, grid=(count,), in_specs=specs)(*operands)

    for role in range(n_roles):
        pl.when(off_ref[2] == role)(functools.partial(run, role))
    out_ref[...] = acc_ref[...].astype(out_ref.dtype)


def down(group, weight, offsets, unit, total, dtype):
    n_roles = len(group[0][2])
    rows, width = group[0][2][0][0].shape[0], weight.shape[1]
    steps, at = [], 0
    for flow in range(2):
        for chunk, (_, size, _, _) in enumerate(group):
            steps.append((flow, chunk, at, size))
            at += size
    pieces = [piece for chunk in group for flow in range(2) for piece in chunk[2 + flow]]
    starts = [chunk[0] for chunk in group]
    extra = () if total is None else (total,)
    return pl.pallas_call(
        functools.partial(
            down_kernel, steps, starts, [place for _, place in pieces], unit, n_roles, total is not None
        ),
        in_specs=[SMEM, HBM] + [ANY] * len(pieces) + [VMEM for _ in extra],
        out_specs=VMEM,
        scratch_shapes=[pltpu.VMEM((rows, width), jnp.float32)],
        out_shape=jax.ShapeDtypeStruct((rows, width), dtype),
        compiler_params=pltpu.CompilerParams(vmem_limit_bytes=KERNEL_VMEM),
        cost_estimate=pl.CostEstimate(
            flops=2 * rows * width * at * unit,
            bytes_accessed=2 * width * at * unit,
            transcendentals=0,
        ),
    )(offsets, weight, *[message for message, _ in pieces], *extra)


def exchange_kernel(jobs, unit, n_in, role_ref, *refs):
    ins, outs = refs[:n_in], refs[n_in:]
    role = role_ref[2]

    def columns(place, size):
        return slice(place * unit, (place + size) * unit)

    def write(out, items, r):
        here = pl.ds(pl.multiple_of(r * ROW_TILE, ROW_TILE), ROW_TILE)
        for kind, place, size, part, came, came_at, scale in items:
            if kind == "sum":
                value = ins[part][here, :]
                if came is not None:
                    value = value.astype(jnp.float32) + ins[came][here, columns(came_at, 2 * size)].astype(jnp.float32)
                out[here, columns(place, 2 * size)] = value.astype(jnp.bfloat16)
            elif kind == "pass":
                out[here, columns(place, size)] = ins[came][here, columns(came_at, size)]
            else:
                for u in range(size):
                    def total(at):
                        both = ins[part][here, columns(at, 1)].astype(jnp.float32)
                        both += ins[came][here, columns(came_at + at, 1)].astype(jnp.float32)
                        return both * ins[scale][here, :]

                    gate, up = total(2 * u), total(2 * u + 1)
                    out[here, columns(place + u, 1)] = (jax.nn.silu(gate) * up).astype(jnp.bfloat16)

    roles = sorted({r for by_role in jobs for r, _ in by_role})
    for which in roles:
        @pl.when(role == which)
        def _():
            @pl.loop(0, outs[0].shape[0] // ROW_TILE)
            def _(r):
                for out, by_role in zip(outs, jobs):
                    for other, items in by_role:
                        if other == which:
                            write(out, items, r)


def exchange(jobs, widths, operands, offsets, unit):
    rows = operands[0].shape[0]
    moved = sum(a.size * a.dtype.itemsize for a in operands) + 2 * rows * sum(widths) * unit
    return pl.pallas_call(
        functools.partial(exchange_kernel, jobs, unit, len(operands)),
        in_specs=[SMEM] + [VMEM] * len(operands),
        out_specs=[VMEM] * len(widths),
        out_shape=[jax.ShapeDtypeStruct((rows, width * unit), jnp.bfloat16) for width in widths],
        compiler_params=pltpu.CompilerParams(vmem_limit_bytes=SMALL_VMEM),
        cost_estimate=pl.CostEstimate(flops=moved, bytes_accessed=moved, transcendentals=0),
    )(offsets, *operands)


def side_pairs(side, count):
    first = [z for z in range(1 - side, count - 1, 2)]
    return [(z, z + 1) for z in first] + [(z + 1, z) for z in first]


def plan(n_pair, units):
    def cut(total, sizes):
        sizes = list(sizes)
        return sizes if sum(sizes) == total else [total]

    head, tail = FIRST, LAST
    if sum(head) + sum(tail) != units:
        head, tail = (1,), (units - 1,)
    chunks, start = [], 0
    for size in head:
        chunks.append((0, start, size))
        start += size
    for pair in range(1, n_pair):
        at = 0
        for size in cut(units, SECOND if pair == 1 else MIDDLE):
            chunks.append((pair, at, size))
            at += size
    for size in tail:
        chunks.append((0, start, size))
        start += size
    return chunks


def body(n_row, n_col, tokens, norm_gain, gate_weight, up_weight, down_weight):
    col = lax.axis_index("col")
    rows, depth = tokens.shape
    half = gate_weight.shape[1] // 2
    unit = 256 if half % 256 == 0 else 128
    units = half // unit
    hops, mid = n_col - 1, n_col // 2

    low = col < mid
    far_at = jnp.where(low, units, 0)
    from_end = jnp.minimum(col, n_col - 1 - col)
    offsets = jnp.stack([far_at, units - far_at, from_end]).astype(jnp.int32)

    n_pair = n_row // 2
    chunks = plan(n_pair, units)
    count = len(chunks)
    first_use = {}
    for i, (pair, _, _) in enumerate(chunks):
        first_use.setdefault(pair, i)

    when = [[None] + [i + h for h in range(2 * hops + 1)] for i in range(count)]
    last_step = when[-1][-1]

    place, width = {}, {}
    for t in range(last_step + 1):
        for h in range(1, hops + 1):
            at = 0
            for kind, shift, scale in (("sum", 0, 2), ("hid", hops, 1)):
                for i in range(count):
                    if when[i][h + shift] == t:
                        place[kind, h, i] = at
                        at += scale * chunks[i][2]
            if at:
                width[t, h] = at

    groups, due = {}, {}
    for i, (pair, _, _) in enumerate(chunks):
        arrival = when[i][-1]
        if pair:
            arrival = max(when[j][-1] for j in range(count) if chunks[j][0] == pair)
        elif i < count // 2:
            arrival = max(when[j][-1] for j in range(count // 2) if chunks[j][0] == pair)
        groups.setdefault((arrival, pair), []).append(i)
    for arrival, pair in groups:
        due[pair] = max(due.get(pair, 0), arrival)

    def sends_of(side):
        hops_of = [(e, e + 1 if (e + 1) % 2 == side else n_col - e) for e in range(mid)]
        return [(e, h) for e, h in hops_of if h < n_col]

    def along_row(value, mask):
        return lax.ppermute(value, "row", [(r, r ^ mask) for r in range(n_row)])

    def along_col(value, mask):
        return lax.ppermute(value, "col", [(c, c ^ mask) for c in range(n_col)])

    def start_chunk(i, x):
        _, start, blocks = chunks[i]
        return gate_up(x, gate_weight, up_weight, offsets, start, blocks, unit)

    own = tokens.astype(jnp.float32)
    gained = (own * norm_gain[None, :]).astype(jnp.bfloat16)
    squares = jnp.sum(own * own, axis=1)[None, :]
    lhs = {0: jnp.concatenate([gained, along_row(gained, 1)], axis=0)}
    scales = {}

    col_masks = [1 << b for b in range(n_col.bit_length() - 1)]
    far, near, came, sent, totals, outs = {}, {}, {}, {}, {}, {}
    far[0], near[0] = start_chunk(0, lhs[0])
    carried = {}
    for t in range(last_step + 1):
        jobs, widths, sides, operands, known = [], [], [], [], {}
        messages = {}

        def operand(name, value):
            if name not in known:
                known[name] = len(operands)
                operands.append(value)
            return known[name]

        def received(h, i, shift):
            before = (when[i][h + shift], h % 2)
            return operand(before, came[before]), place["hid" if shift else "sum", h, i]

        for side in (1, 0):
            active = [(e, h) for e, h in sends_of(side) if (t, h) in width]
            if not active:
                continue
            by_role = []
            for e, h in active:
                items = []
                for i in range(count):
                    size = chunks[i][2]
                    if when[i][h] == t:
                        mine = ("far", i) if h <= mid else ("near", i)
                        part = operand(mine, (far if h <= mid else near)[i])
                        old = received(h - 1, i, 0) if h > 1 else (None, 0)
                        items.append(("sum", place["sum", h, i], size, part, *old, None))
                    if when[i][h + hops] == t and h == 1:
                        pair = chunks[i][0]
                        part, old = operand(("near", i), near[i]), received(hops, i, 0)
                        scale = operand(("scale", pair), scales[pair].reshape(2 * rows, 1))
                        items.append(("hid", place["hid", h, i], size, part, *old, scale))
                    elif when[i][h + hops] == t:
                        old = received(h - 1, i, hops)
                        items.append(("pass", place["hid", h, i], size, None, *old, None))
                by_role.append((e, items))
            only = by_role[0][1][0] if len(by_role) == len(by_role[0][1]) == 1 else None
            if only and only[0] == "sum" and only[4] is None:
                messages[side] = operands[only[3]]
            else:
                jobs.append(by_role)
                sides.append(side)
                widths.append(max(width[t, h] for _, h in active))
        if jobs:
            messages.update(zip(sides, exchange(jobs, widths, operands, offsets, unit)))

        extra = {}
        wanted = [pair for pair in range(1, n_pair) if max(0, first_use[pair] - AHEAD) == t]
        if wanted:
            extra["gained"] = lhs[0]
        if t + 1 < count:
            extra["x"] = lhs[chunks[t + 1][0]]
        if t <= len(col_masks) + 1:
            extra["squares"] = squares
        arrived = [(pair, members) for (arrival, pair), members in groups.items() if arrival == t]
        for pair, members in arrived:
            for i in members:
                for h in range(1, hops + 1):
                    key = (when[i][h + hops], h % 2)
                    extra["came", key] = came[key]
        extra.update(carried)
        carried = {}

        values = lax.optimization_barrier((list(messages.values()), list(extra.values())))
        messages, extra = dict(zip(messages, values[0])), dict(zip(extra, values[1]))
        for key in [key for key in extra if isinstance(key, tuple) and key[0] == "total"]:
            totals[key] = extra[key]
        for side, value in messages.items():
            came[t, side] = lax.ppermute(value, "col", side_pairs(side, n_col))
            sent[t, side] = value
        for pair in wanted:
            lhs[pair] = along_row(extra["gained"], 2 * pair)
        if t < len(col_masks):
            squares = extra["squares"] + along_col(extra["squares"], col_masks[t])
        elif t == len(col_masks):
            scale = lax.rsqrt(extra["squares"] / (depth * n_col) + 1e-05)
            squares = scales[0] = jnp.concatenate([scale, along_row(scale, 1)], axis=0)
        elif t == len(col_masks) + 1:
            for pair in range(1, n_pair):
                scales[pair] = along_row(extra["squares"], 2 * pair)
        if "x" in extra:
            far[t + 1], near[t + 1] = start_chunk(t + 1, extra["x"])
        for pair, members in arrived:
            group = []
            for i in members:
                def hidden(h):
                    if h == 0:
                        return sent[when[i][1 + hops], 1], place["hid", 1, i]
                    return extra["came", (when[i][h + hops], h % 2)], place["hid", h, i]

                roles = range(mid)
                group.append((
                    chunks[i][1], chunks[i][2],
                    [hidden(e) for e in roles], [hidden(n_col - 1 - e) for e in roles],
                ))
            last = due[pair] == t
            result = down(
                group, down_weight, offsets, unit, totals.pop(("total", pair), None),
                jnp.bfloat16 if last and pair else jnp.float32,
            )
            if not last:
                carried["total", pair] = result
            elif pair == 0:
                outs[pair] = result
            else:
                outs[pair] = along_row(result, 2 * pair)
    mixed = functools.reduce(jnp.add, [outs[pair].astype(jnp.float32) for pair in range(n_pair)])
    other = along_row(mixed[rows:].astype(jnp.bfloat16), 1)
    return (mixed[:rows] + other.astype(jnp.float32)).astype(jnp.bfloat16)


def solution(mesh):
    placed = (P("row", "col"), P("col"), P("col", "row"), P("col", "row"), P("row", "col"))
    n_row, n_col = mesh.shape["row"], mesh.shape["col"]
    return jax.shard_map(
        functools.partial(body, n_row, n_col),
        mesh=mesh, in_specs=placed, out_specs=P("row", "col"), check_vma=False,
    )
```

```python
import functools

import jax
import jax.numpy as jnp
from jax import lax
from jax.experimental import pallas as pl
from jax.experimental.pallas import tpu as pltpu
from jax.sharding import PartitionSpec as P


FIRST = (2, 2)
SECOND = (4, 3)
MIDDLE = (4, 3)
LAST = (2, 1)
AHEAD = 3
ROW_TILE = 32
DOWN_TILE = 512
KERNEL_VMEM = 52 * 2**20
SMALL_VMEM = 8 * 2**20


HBM = pl.BlockSpec(memory_space=pltpu.HBM)
VMEM = pl.BlockSpec(memory_space=pltpu.VMEM)
SMEM = pl.BlockSpec(memory_space=pltpu.SMEM)
ANY = pl.BlockSpec(memory_space=pl.ANY)


def gate_up_kernel(blocks, start, unit, off_ref, x_ref, gate_hbm, up_hbm, far_ref, near_ref):
    wide = 2 if blocks % 2 == 0 else 1
    per_flow = blocks // wide

    def step(gate_ref, up_ref):
        i = pl.program_id(0)
        x = x_ref[...]
        gate = jnp.dot(x, gate_ref[...], preferred_element_type=jnp.float32).astype(jnp.bfloat16)
        up = jnp.dot(x, up_ref[...], preferred_element_type=jnp.float32).astype(jnp.bfloat16)

        def write(ref, block):
            for w in range(wide):
                at = pl.multiple_of(2 * unit * (wide * block + w), 2 * unit)
                ref[:, pl.ds(at, unit)] = gate[:, w * unit : (w + 1) * unit]
                ref[:, pl.ds(at + unit, unit)] = up[:, w * unit : (w + 1) * unit]

        pl.when(i < per_flow)(lambda: write(far_ref, i))
        pl.when(i >= per_flow)(lambda: write(near_ref, i - per_flow))

    depth = x_ref.shape[1]
    if wide == 1:
        weight = pl.BlockSpec(
            (depth, unit), lambda i: (0, off_ref[i // blocks] + start + i - (i // blocks) * blocks)
        )
        pltpu.emit_pipeline(step, grid=(2 * blocks,), in_specs=[weight, weight])(gate_hbm, up_hbm)
        return
    weight = pl.BlockSpec(
        (pl.Element(depth), pl.Element(wide * unit)),
        lambda i: (0, pl.multiple_of(
            (off_ref[i // per_flow] + start + wide * (i - (i // per_flow) * per_flow)) * unit, unit)),
    )
    pltpu.emit_pipeline(step, grid=(2 * per_flow,), in_specs=[weight, weight])(gate_hbm, up_hbm)


def gate_up(x, gate_weight, up_weight, offsets, start, blocks, unit):
    rows, depth = x.shape
    shape = jax.ShapeDtypeStruct((rows, 2 * blocks * unit), jnp.bfloat16)
    return pl.pallas_call(
        functools.partial(gate_up_kernel, blocks, start, unit),
        in_specs=[SMEM, VMEM, HBM, HBM],
        out_specs=[VMEM, VMEM],
        out_shape=[shape, shape],
        compiler_params=pltpu.CompilerParams(vmem_limit_bytes=KERNEL_VMEM),
        cost_estimate=pl.CostEstimate(
            flops=8 * rows * depth * blocks * unit,
            bytes_accessed=8 * depth * blocks * unit,
            transcendentals=0,
        ),
    )(offsets, x, gate_weight, up_weight)


def down_kernel(parts, unit, tile, n_roles, has_total, off_ref, weight_hbm, *refs):
    out_hbm = refs[-1]
    rows, width = out_hbm.shape
    column = pl.BlockSpec((rows, tile), lambda j: (0, j))

    def run(role):
        weights, hidden, specs = [], [], []
        for p, (flow, start, size, places) in enumerate(parts):
            first = pl.multiple_of((off_ref[1 - flow] + start) * unit, unit)
            weights.append(weight_hbm.at[pl.ds(first, size * unit), :])
            hidden.append(refs[p * n_roles + role].at[:, pl.ds(places[role] * unit, size * unit)])
            specs.append(pl.BlockSpec((size * unit, tile), lambda j: (0, j)))
        specs += [pl.BlockSpec((rows, size * unit), lambda j: (0, 0)) for _, _, size, _ in parts]
        extra = [refs[-2]] if has_total else []

        def step(*blocks):
            total = blocks[2 * len(parts)][...] if has_total else None
            for weight, value in zip(blocks[: len(parts)], blocks[len(parts) :]):
                part = jnp.dot(value[...], weight[...], preferred_element_type=jnp.float32)
                total = part if total is None else total + part
            blocks[-1][...] = total.astype(blocks[-1].dtype)

        pltpu.emit_pipeline(
            step, grid=(width // tile,), in_specs=specs + [column for _ in extra], out_specs=[column]
        )(*weights, *hidden, *extra, out_hbm)

    for role in range(n_roles):
        pl.when(off_ref[2] == role)(functools.partial(run, role))


def down(group, weight, offsets, unit, total, dtype):
    n_roles = len(group[0][2])
    rows, width = group[0][2][0][0].shape[0], weight.shape[1]
    parts, pieces = [], []
    for start, size, *flows in group:
        for flow, by_role in enumerate(flows):
            parts.append((flow, start, size, [place for _, place in by_role]))
            pieces += [message for message, _ in by_role]
    depth = unit * sum(size for _, _, size, _ in parts)
    extra = () if total is None else (total,)
    return pl.pallas_call(
        functools.partial(down_kernel, parts, unit, min(DOWN_TILE, width), n_roles, total is not None),
        in_specs=[SMEM, HBM] + [ANY] * (len(pieces) + len(extra)),
        out_specs=ANY,
        out_shape=jax.ShapeDtypeStruct((rows, width), dtype),
        compiler_params=pltpu.CompilerParams(vmem_limit_bytes=KERNEL_VMEM),
        cost_estimate=pl.CostEstimate(
            flops=2 * rows * width * depth, bytes_accessed=2 * width * depth, transcendentals=0
        ),
    )(offsets, weight, *pieces, *extra)


def exchange_kernel(jobs, unit, n_in, role_ref, *refs):
    ins, outs = refs[:n_in], refs[n_in:]
    role = role_ref[2]

    def columns(place, size):
        return slice(place * unit, (place + size) * unit)

    def write(out, items, r):
        here = pl.ds(pl.multiple_of(r * ROW_TILE, ROW_TILE), ROW_TILE)
        for kind, place, size, part, came, came_at, scale in items:
            if kind == "sum":
                value = ins[part][here, :]
                if came is not None:
                    value = value.astype(jnp.float32) + ins[came][here, columns(came_at, 2 * size)].astype(jnp.float32)
                out[here, columns(place, 2 * size)] = value.astype(jnp.bfloat16)
            elif kind == "pass":
                out[here, columns(place, size)] = ins[came][here, columns(came_at, size)]
            else:
                for u in range(size):
                    def total(at):
                        both = ins[part][here, columns(at, 1)].astype(jnp.float32)
                        both += ins[came][here, columns(came_at + at, 1)].astype(jnp.float32)
                        return both * ins[scale][here, :]

                    gate, up = total(2 * u), total(2 * u + 1)
                    out[here, columns(place + u, 1)] = (jax.nn.silu(gate) * up).astype(jnp.bfloat16)

    roles = sorted({r for by_role in jobs for r, _ in by_role})
    for which in roles:
        @pl.when(role == which)
        def _():
            @pl.loop(0, outs[0].shape[0] // ROW_TILE)
            def _(r):
                for out, by_role in zip(outs, jobs):
                    for other, items in by_role:
                        if other == which:
                            write(out, items, r)


def exchange(jobs, widths, operands, offsets, unit):
    rows = operands[0].shape[0]
    moved = sum(a.size * a.dtype.itemsize for a in operands) + 2 * rows * sum(widths) * unit
    return pl.pallas_call(
        functools.partial(exchange_kernel, jobs, unit, len(operands)),
        in_specs=[SMEM] + [VMEM] * len(operands),
        out_specs=[VMEM] * len(widths),
        out_shape=[jax.ShapeDtypeStruct((rows, width * unit), jnp.bfloat16) for width in widths],
        compiler_params=pltpu.CompilerParams(vmem_limit_bytes=SMALL_VMEM),
        cost_estimate=pl.CostEstimate(flops=moved, bytes_accessed=moved, transcendentals=0),
    )(offsets, *operands)


def side_pairs(side, count):
    first = [z for z in range(1 - side, count - 1, 2)]
    return [(z, z + 1) for z in first] + [(z + 1, z) for z in first]


def plan(n_pair, units):
    def cut(total, sizes):
        sizes = list(sizes)
        return sizes if sum(sizes) == total else [total]

    head, tail = FIRST, LAST
    if sum(head) + sum(tail) != units:
        head, tail = (1,), (units - 1,)
    chunks, start = [], 0
    for size in head:
        chunks.append((0, start, size))
        start += size
    for pair in range(1, n_pair):
        at = 0
        for size in cut(units, SECOND if pair == 1 else MIDDLE):
            chunks.append((pair, at, size))
            at += size
    for size in tail:
        chunks.append((0, start, size))
        start += size
    return chunks


def body(n_row, n_col, tokens, norm_gain, gate_weight, up_weight, down_weight):
    col = lax.axis_index("col")
    rows, depth = tokens.shape
    half = gate_weight.shape[1] // 2
    unit = 256 if half % 256 == 0 else 128
    units = half // unit
    hops, mid = n_col - 1, n_col // 2

    low = col < mid
    far_at = jnp.where(low, units, 0)
    from_end = jnp.minimum(col, n_col - 1 - col)
    offsets = jnp.stack([far_at, units - far_at, from_end]).astype(jnp.int32)

    n_pair = n_row // 2
    chunks = plan(n_pair, units)
    count = len(chunks)
    first_use = {}
    for i, (pair, _, _) in enumerate(chunks):
        first_use.setdefault(pair, i)

    when = [[None] + [i + h for h in range(2 * hops + 1)] for i in range(count)]
    last_step = when[-1][-1]

    place, width = {}, {}
    for t in range(last_step + 1):
        for h in range(1, hops + 1):
            at = 0
            for kind, shift, scale in (("sum", 0, 2), ("hid", hops, 1)):
                for i in range(count):
                    if when[i][h + shift] == t:
                        place[kind, h, i] = at
                        at += scale * chunks[i][2]
            if at:
                width[t, h] = at

    groups, due = {}, {}
    for i, (pair, _, _) in enumerate(chunks):
        arrival = when[i][-1]
        if 0 < pair < n_pair - 1:
            arrival = max(when[j][-1] for j in range(count) if chunks[j][0] == pair)
        elif pair == 0 and i < count // 2:
            arrival = max(when[j][-1] for j in range(count // 2) if chunks[j][0] == pair)
        groups.setdefault((arrival, pair), []).append(i)
    for arrival, pair in groups:
        due[pair] = max(due.get(pair, 0), arrival)

    def sends_of(side):
        hops_of = [(e, e + 1 if (e + 1) % 2 == side else n_col - e) for e in range(mid)]
        return [(e, h) for e, h in hops_of if h < n_col]

    def along_row(value, mask):
        return lax.ppermute(value, "row", [(r, r ^ mask) for r in range(n_row)])

    def along_col(value, mask):
        return lax.ppermute(value, "col", [(c, c ^ mask) for c in range(n_col)])

    def start_chunk(i, x):
        _, start, blocks = chunks[i]
        return gate_up(x, gate_weight, up_weight, offsets, start, blocks, unit)

    own = tokens.astype(jnp.float32)
    gained = (own * norm_gain[None, :]).astype(jnp.bfloat16)
    squares = jnp.sum(own * own, axis=1)[None, :]
    lhs = {0: jnp.concatenate([gained, along_row(gained, 1)], axis=0)}
    scales = {}

    col_masks = [1 << b for b in range(n_col.bit_length() - 1)]
    far, near, came, sent, totals, outs = {}, {}, {}, {}, {}, {}
    if n_pair > 1:
        lhs[1] = along_row(lhs[0], 2)
    squares = squares + along_col(squares, col_masks[0])
    far[0], near[0] = start_chunk(0, lhs[0])
    stages = {t: mask for t, mask in enumerate(col_masks[1:])}
    ready = max(2, len(col_masks) - 1)
    stages[ready], stages[ready + 1] = "core", "row"
    carried = {}
    for t in range(last_step + 1):
        jobs, widths, sides, operands, known = [], [], [], [], {}
        messages = {}

        def operand(name, value):
            if name not in known:
                known[name] = len(operands)
                operands.append(value)
            return known[name]

        def received(h, i, shift):
            before = (when[i][h + shift], h % 2)
            return operand(before, came[before]), place["hid" if shift else "sum", h, i]

        for side in (1, 0):
            active = [(e, h) for e, h in sends_of(side) if (t, h) in width]
            if not active:
                continue
            by_role = []
            for e, h in active:
                items = []
                for i in range(count):
                    size = chunks[i][2]
                    if when[i][h] == t:
                        mine = ("far", i) if h <= mid else ("near", i)
                        part = operand(mine, (far if h <= mid else near)[i])
                        old = received(h - 1, i, 0) if h > 1 else (None, 0)
                        items.append(("sum", place["sum", h, i], size, part, *old, None))
                    if when[i][h + hops] == t and h == 1:
                        pair = chunks[i][0]
                        part, old = operand(("near", i), near[i]), received(hops, i, 0)
                        scale = operand(("scale", pair), scales[pair].reshape(2 * rows, 1))
                        items.append(("hid", place["hid", h, i], size, part, *old, scale))
                    elif when[i][h + hops] == t:
                        old = received(h - 1, i, hops)
                        items.append(("pass", place["hid", h, i], size, None, *old, None))
                by_role.append((e, items))
            only = by_role[0][1][0] if len(by_role) == len(by_role[0][1]) == 1 else None
            if only and only[0] == "sum" and only[4] is None:
                messages[side] = operands[only[3]]
            else:
                jobs.append(by_role)
                sides.append(side)
                widths.append(max(width[t, h] for _, h in active))
        if jobs:
            messages.update(zip(sides, exchange(jobs, widths, operands, offsets, unit)))

        extra = {}
        wanted = [pair for pair in range(2, n_pair) if max(0, first_use[pair] - AHEAD) == t]
        if wanted:
            extra["gained"] = lhs[0]
        stage = stages.get(t)
        if stage:
            extra["squares"] = squares
        arrived = [(pair, members) for (arrival, pair), members in groups.items() if arrival == t]
        for pair, members in arrived:
            for i in members:
                for h in range(1, hops + 1):
                    key = (when[i][h + hops], h % 2)
                    extra["came", key] = came[key]
        extra.update(carried)
        carried = {}

        values = lax.optimization_barrier((list(messages.values()), list(extra.values())))
        messages, extra = dict(zip(messages, values[0])), dict(zip(extra, values[1]))
        for key in [key for key in extra if isinstance(key, tuple) and key[0] == "total"]:
            totals[key] = extra[key]
        for side, value in messages.items():
            came[t, side] = lax.ppermute(value, "col", side_pairs(side, n_col))
            sent[t, side] = value
        for pair in wanted:
            lhs[pair] = along_row(extra["gained"], 2 * pair)
        if stage == "core":
            scale = lax.rsqrt(extra["squares"] / (depth * n_col) + 1e-05)
            squares = scales[0] = jnp.concatenate([scale, along_row(scale, 1)], axis=0)
        elif stage == "row":
            for pair in range(1, n_pair):
                scales[pair] = along_row(extra["squares"], 2 * pair)
        elif stage:
            squares = extra["squares"] + along_col(extra["squares"], stage)
        if t + 1 < count:
            far[t + 1], near[t + 1] = start_chunk(t + 1, lhs[chunks[t + 1][0]])
        for pair, members in arrived:
            group = []
            for i in members:
                def hidden(h):
                    if h == 0:
                        return sent[when[i][1 + hops], 1], place["hid", 1, i]
                    return extra["came", (when[i][h + hops], h % 2)], place["hid", h, i]

                roles = range(mid)
                group.append((
                    chunks[i][1], chunks[i][2],
                    [hidden(e) for e in roles], [hidden(n_col - 1 - e) for e in roles],
                ))
            last = due[pair] == t
            result = down(
                group, down_weight, offsets, unit, totals.pop(("total", pair), None),
                jnp.bfloat16 if last and pair else jnp.float32,
            )
            if not last:
                carried["total", pair] = result
            elif pair == 0:
                outs[pair] = result
            else:
                outs[pair] = along_row(result, 2 * pair)
    mixed = functools.reduce(jnp.add, [outs[pair].astype(jnp.float32) for pair in range(n_pair)])
    other = along_row(mixed[rows:].astype(jnp.bfloat16), 1)
    return (mixed[:rows] + other.astype(jnp.float32)).astype(jnp.bfloat16)


def solution(mesh):
    placed = (P("row", "col"), P("col"), P("col", "row"), P("col", "row"), P("row", "col"))
    n_row, n_col = mesh.shape["row"], mesh.shape["col"]
    return jax.shard_map(
        functools.partial(body, n_row, n_col),
        mesh=mesh, in_specs=placed, out_specs=P("row", "col"), check_vma=False,
    )
```
